32 devices in a mesh: py: 8 (over y, x, core), pz: 4 (over z).
Axes of the slice: x: 2, y: 2, z: 4, core: 2. Of those that a mesh axis runs over, the one named last changes fastest.
Arguments:
- velocity: float32 [3, 320, 320, 320], P(None, 'py', 'pz'), may hold values from -12 to 12
Outputs:
- filtered_velocity: float32 [3, 128, 128, 128], P(None, 'py', 'pz')
- subgrid_stress: float32 [6, 128, 128, 128], P(None, 'py', 'pz')
The draws below stay inside these ranges and needn't reach their ends.
All inputs are finite; a program needn't handle non-finite values.
Results may differ from the reference program's by a relative error of at most 0.000082.
Values sent between devices are 32-bit elements; how exact they have to be, the bound alone decides.
A program may use at most 128 MiB of HBM per device.

```python
import math
import jax
import jax.numpy as jnp

N = 320
M = 128


def block_levels(own_key, shape, pieces, least, largest):
    factor_of = 1.0
    for axis_at, parts in pieces:
        heights = jax.random.uniform(jax.random.fold_in(jax.random.fold_in(own_key, 6), axis_at), (parts,), jnp.float32, least / len(pieces), largest / len(pieces))
        factor_of = factor_of * jnp.repeat(jnp.exp(heights), shape[axis_at] // parts).reshape((-1,) + (1,) * (len(shape) - 1 - axis_at))
    return factor_of


def normal_values(rng, shape, spread, reach, shards=(), kind=jnp.bfloat16):
    drawn = jax.random.normal(rng, shape, jnp.float32) * spread
    if len(shards) > 0:
        drawn = block_levels(rng, shape, shards, -0.22, 0.18) * drawn
    return jnp.clip(drawn, min=-reach, max=reach).astype(kind)


def setup_inputs(seed: int = 0) -> dict:
    keys = jax.random.split(jax.random.key(seed), 2)
    return {
        "velocity": normal_values(keys[0], (3, N, N, N), 2.0, 12.0, ((1, 8), (2, 4)), jnp.float32),
    }


factor_pairs = ((0, 0), (0, 1), (0, 2), (1, 1), (1, 2), (2, 2))


def kept_indices():
    return jnp.concatenate([jnp.arange(M // 2, dtype=jnp.int32), jnp.arange(N - M // 2, N, dtype=jnp.int32)])


def filter_values():
    half_modes = M // 2
    signed_modes = jnp.concatenate([jnp.arange(half_modes, dtype=jnp.int32), jnp.arange(half_modes, dtype=jnp.int32) - half_modes])
    wave_numbers = signed_modes.astype(jnp.float32)
    squares = wave_numbers[:, None, None] ** 2 + wave_numbers[None, :, None] ** 2 + wave_numbers[None, None, :] ** 2
    valid_modes = signed_modes != -half_modes
    retained = valid_modes[:, None, None] & valid_modes[None, :, None] & valid_modes[None, None, :]
    filter_width = 2.0 * math.pi / M
    return jnp.where(retained, jnp.exp(-squares * (filter_width * filter_width / 24.0)), 0.0).astype(jnp.float32)


def filtered_field(fine_field, gain_table, kept_modes):
    spectrum = jnp.take(jnp.fft.fft(fine_field, axis=2), kept_modes, axis=2)
    spectrum = jnp.take(jnp.fft.fft(spectrum, axis=1), kept_modes, axis=1)
    spectrum = jnp.take(jnp.fft.fft(spectrum, axis=0), kept_modes, axis=0)
    coarse = jnp.real(jnp.fft.ifftn(spectrum * gain_table)) * (float(M) ** 3 / float(N) ** 3)
    return jnp.transpose(coarse, (1, 2, 0)).astype(jnp.float32)


def reference(velocity):
    gain_table = filter_values()
    kept_modes = kept_indices()
    coarse = [filtered_field(velocity[component], gain_table, kept_modes) for component in range(3)]
    products = [filtered_field(velocity[left_index] * velocity[right_index], gain_table, kept_modes) for left_index, right_index in factor_pairs]
    filtered = jnp.stack(coarse)
    stress = jnp.stack([products[position] - coarse[left_index] * coarse[right_index] for position, (left_index, right_index) in enumerate(factor_pairs)])
    return filtered, stress
```

```python
import math

import jax
import jax.numpy as jnp
import numpy as np
from jax import lax
from jax.sharding import PartitionSpec as P

factor_pairs = ((0, 0), (0, 1), (0, 2), (1, 1), (1, 2), (2, 2))


def line_filter(fine, coarse):
    half = coarse // 2
    modes = np.arange(1, half)
    width = 2.0 * math.pi / coarse
    gain = np.exp(-(modes.astype(np.float64) ** 2) * (width * width / 24.0))
    turns = np.arange(coarse)[:, None] * fine - np.arange(fine)[None, :] * coarse
    period = fine * coarse
    matrix = np.ones((coarse, fine))
    for mode, weight in zip(modes, gain):
        matrix += 2.0 * weight * np.cos(2.0 * math.pi * ((mode * turns) % period) / period)
    return (matrix / fine).astype(np.float32)


def shards(velocity):
    fine = velocity.shape[3]
    coarse_size = fine * 2 // 5
    matrix = jnp.asarray(line_filter(fine, coarse_size))
    components = [velocity[component] for component in range(3)]
    fields = jnp.stack(components + [components[a] * components[b] for a, b in factor_pairs])
    high = lax.Precision.HIGH
    third = jnp.einsum("fabk,mk->fabm", fields, matrix, precision=high)
    third = lax.all_to_all(third, "pz", split_axis=3, concat_axis=2, tiled=True)
    second = jnp.einsum("fabm,nb->fanm", third, matrix, precision=high)
    second = lax.all_to_all(second, "py", split_axis=2, concat_axis=1, tiled=True)
    coarse = jnp.einsum("fanm,pa->fnmp", second, matrix, precision=high)
    stress = jnp.stack(
        [coarse[3 + p] - coarse[a] * coarse[b] for p, (a, b) in enumerate(factor_pairs)]
    )
    return coarse[:3], stress


def solution(mesh):
    placed = P(None, "py", "pz", None)
    return jax.shard_map(
        shards, mesh=mesh, in_specs=(placed,), out_specs=(placed, placed), check_vma=False
    )
```

```python
import functools
import math

import jax
import jax.numpy as jnp
import ml_dtypes
import numpy as np
from jax import lax
from jax.experimental import pallas as pl
from jax.experimental.pallas import tpu as pltpu
from jax.sharding import PartitionSpec as P

M = 128

factor_pairs = ((0, 0), (0, 1), (0, 2), (1, 1), (1, 2), (2, 2))
fields_count = 9
LANES = 128


def line_filter(fine, coarse):
    half = coarse // 2
    modes = np.arange(1, half)
    width = 2.0 * math.pi / coarse
    gain = np.exp(-(modes.astype(np.float64) ** 2) * (width * width / 24.0))
    turns = np.arange(coarse)[:, None] * fine - np.arange(fine)[None, :] * coarse
    period = fine * coarse
    matrix = np.ones((coarse, fine))
    for mode, weight in zip(modes, gain):
        matrix += 2.0 * weight * np.cos(2.0 * math.pi * ((mode * turns) % period) / period)
    return (matrix / fine).astype(np.float32)


def halves(matrix):
    top = matrix.astype(ml_dtypes.bfloat16)
    return top, (matrix - top.astype(np.float32)).astype(ml_dtypes.bfloat16)


def split(value):
    top = value.astype(jnp.bfloat16)
    return top, (value - top.astype(jnp.float32)).astype(jnp.bfloat16)


def dot(left, right):
    return jnp.dot(left, right, preferred_element_type=jnp.float32)


def rows_times(value, table):
    width = table.shape[1] // 2
    top, rest = split(value)
    both = dot(top, table)
    return both[:, :width] + both[:, width:] + dot(rest, table[:, :width])


def kernel(
    rows, columns, velocity, third, second, first, filtered, stress,
    fine, lines, send_z, recv_z, send_y, recv_y, turned,
    load_sem, send_z_sem, recv_z_sem, send_y_sem, recv_y_sem,
):
    me_y = lax.axis_index("py")
    me_z = lax.axis_index("pz")
    steps = fine.shape[1]
    depth = fine.shape[3]
    block = LANES // columns
    band = filtered.shape[1]
    MESH = pl.DeviceIdType.MESH

    def load(c):
        return pltpu.make_async_copy(velocity.at[c], fine.at[c], load_sem.at[c])

    for c in range(3):
        load(c).start()

    barrier = pltpu.get_barrier_semaphore()
    for k in range(1, columns):
        pl.semaphore_signal(
            barrier, inc=1, device_id=(me_y, (me_z + k) % columns), device_id_type=MESH
        )
    for j in range(1, rows):
        pl.semaphore_signal(
            barrier, inc=1, device_id=((me_y + j) % rows, me_z), device_id_type=MESH
        )
    pl.semaphore_wait(barrier, columns + rows - 2)

    def copy_z(f, k):
        return pltpu.make_async_remote_copy(
            src_ref=send_z.at[f, k - 1],
            dst_ref=recv_z.at[f, k],
            send_sem=send_z_sem.at[f, k - 1],
            recv_sem=recv_z_sem.at[f, k - 1],
            device_id=(me_y, (me_z + k) % columns),
            device_id_type=MESH,
        )

    def copy_y(f, j):
        return pltpu.make_async_remote_copy(
            src_ref=send_y.at[f, j - 1],
            dst_ref=recv_y.at[f, pl.ds(j * steps, steps)],
            send_sem=send_y_sem.at[f, j - 1],
            recv_sem=recv_y_sem.at[f, j - 1],
            device_id=((me_y + rows - j) % rows, me_z),
            device_id_type=MESH,
        )

    def pair_of(f):
        return f // 6 + f // 8, f - 3 - 2 * (f // 6) - f // 8

    half = steps // 2

    def contract_third(f, product):
        if product:
            left, right = pair_of(f)
        else:
            left = right = f

        def piece(t, carry):
            b, h = t // 2, t % 2
            where = pl.ds(h * half, half)
            value = fine[left, where, b]
            if product:
                value = value * fine[right, where, b]
            value = value.reshape(half * depth, value.shape[-1])
            out = rows_times(value, third[b])
            lines[b, where] = out.reshape(half, depth, LANES)
            return carry

        lax.fori_loop(0, columns * 2, piece, 0)

        def regroup(a, carry):
            group = lax.broadcasted_iota(jnp.int32, (depth, LANES), 1) // block
            parts = [lines[b, a] for b in range(columns)]
            for k in range(columns):
                out = parts[-1]
                for b in range(columns - 1):
                    out = jnp.where(group == (me_z + k + b) % columns, parts[b], out)
                if k == 0:
                    recv_z[f, 0, a] = out
                else:
                    send_z[f, k - 1, a] = out
            return carry

        lax.fori_loop(0, steps, regroup, 0)
        for k in range(1, columns):
            copy_z(f, k).start()

    def contract_second(f):
        for k in range(1, columns):
            copy_z(f, k).wait_recv()

        def piece(h, carry):
            value = jnp.concatenate(
                [recv_z[f, :, 2 * h + i].reshape(columns * depth, LANES) for i in range(2)], axis=1
            )
            top, rest = split(value)
            table = second[...]
            both = dot(table, top)
            out = both[:M] + both[M:] + dot(table[:M], rest)
            for i in range(2):
                for j in range(rows):
                    part = out[j * band : (j + 1) * band, i * LANES : (i + 1) * LANES]
                    if j == 0:
                        recv_y[f, 2 * h + i] = part
                    else:
                        send_y[f, j - 1, 2 * h + i] = part
            return carry

        lax.fori_loop(0, half, piece, 0)
        for j in range(1, rows):
            copy_y(f, j).start()

    def contract_first(f, product):
        for j in range(1, rows):
            copy_y(f, j).wait_recv()
        pad = jnp.zeros((LANES - rows * steps, LANES), jnp.float32)
        for m in range(band):
            plane = jnp.concatenate([recv_y[f, :, m, :], pad], axis=0).T
            for g in range(columns):
                turned[m * block : (m + 1) * block, g * LANES : (g + 1) * LANES] = plane[
                    g * block : (g + 1) * block
                ]
        out = rows_times(turned[...], first[...]).reshape(band, block, M)
        if product:
            left, right = pair_of(f)
            stress[f - 3] = out - filtered[left] * filtered[right]
        else:
            filtered[f] = out

    def loop(start, stop, *work):
        def body(f, carry):
            for one in work:
                one(f)
            return carry

        lax.fori_loop(start, stop, body, 0)

    loop(0, 3, lambda f: load(f).wait(), lambda f: contract_third(f, False))
    loop(3, fields_count, lambda f: contract_third(f, True))
    loop(0, 2, contract_second)
    loop(2, 5, contract_second, lambda f: contract_first(f - 2, False))
    loop(5, fields_count, contract_second, lambda f: contract_first(f - 2, True))
    loop(fields_count - 2, fields_count, lambda f: contract_first(f, True))

    def finish(f):
        for k in range(1, columns):
            copy_z(f, k).wait_send()
        for j in range(1, rows):
            copy_y(f, j).wait_send()

    loop(0, fields_count, finish)


def tables(fine, rows, columns):
    matrix = line_filter(fine, M)
    block, band, depth = M // columns, M // rows, fine // columns
    steps = fine // rows // columns
    top, rest = halves(matrix)
    third, second, first = [], [], []
    for b in range(columns):
        order = np.concatenate(
            [np.arange(block) + ((g - b) % columns) * block for g in range(columns)]
        )
        third.append(np.concatenate([top.T[:, order], rest.T[:, order]], axis=1))
    lines = np.concatenate([np.arange(band) + (-r % rows) * band for r in range(2 * rows)])
    for z in range(columns):
        order = np.concatenate(
            [np.arange(depth) + ((z - k) % columns) * depth for k in range(columns)]
        )
        second.append(np.stack([half[lines][:, order] for half in (top, rest)]))
        groups = []
        for g in range(columns):
            points = np.concatenate(
                [
                    (r % rows) * steps * columns + np.arange(steps) * columns + (g - z) % columns
                    for r in range(2 * rows)
                ]
            )
            groups.append(np.concatenate([top.T[points], rest.T[points]], axis=1))
        first.append(np.stack(groups))
    return np.stack(third), np.stack(second), np.stack(first)


def kernel_shards(velocity):
    rows, columns = lax.axis_size("py"), lax.axis_size("pz")
    me_y, me_z = lax.axis_index("py"), lax.axis_index("pz")
    _, lines, depth, fine = velocity.shape
    steps = lines // columns
    block, band = M // columns, M // rows
    third, second, first = tables(fine, rows, columns)
    second = lax.dynamic_slice(
        jnp.asarray(second), (me_z, 0, (rows - me_y) % rows * band, 0), (1, 2, M, fine)
    ).reshape(2 * M, fine)
    first = lax.dynamic_slice(
        jnp.asarray(first), (me_z, 0, me_y * steps, 0), (1, columns, rows * steps, 2 * M)
    )[0]
    first = jnp.pad(first, ((0, 0), (0, LANES - rows * steps), (0, 0)))
    first = first.reshape(columns * LANES, 2 * M)
    velocity = velocity.reshape(3, steps, columns, depth, fine)
    vmem = pl.BlockSpec(memory_space=pltpu.VMEM)
    dma = pltpu.SemaphoreType.DMA
    f32 = jnp.float32
    return pl.pallas_call(
        functools.partial(kernel, rows, columns),
        out_shape=(
            jax.ShapeDtypeStruct((3, band, block, M), f32),
            jax.ShapeDtypeStruct((6, band, block, M), f32),
        ),
        in_specs=[pl.BlockSpec(memory_space=pl.ANY), vmem, vmem, vmem],
        out_specs=(vmem, vmem),
        scratch_shapes=[
            pltpu.VMEM((3, steps, columns, depth, fine), f32),
            pltpu.VMEM((columns, steps, depth, LANES), f32),
            pltpu.VMEM((fields_count, columns - 1, steps, depth, LANES), f32),
            pltpu.VMEM((fields_count, columns, steps, depth, LANES), f32),
            pltpu.VMEM((fields_count, rows - 1, steps, band, LANES), f32),
            pltpu.VMEM((fields_count, rows * steps, band, LANES), f32),
            pltpu.VMEM((band * block, columns * LANES), f32),
            dma((3,)),
            dma((fields_count, columns - 1)),
            dma((fields_count, columns - 1)),
            dma((fields_count, rows - 1)),
            dma((fields_count, rows - 1)),
        ],
        compiler_params=pltpu.CompilerParams(
            collective_id=0, has_side_effects=True, vmem_limit_bytes=67_000_000
        ),
    )(velocity, jnp.asarray(third), second, first)


def plain_shards(velocity):
    matrix = jnp.asarray(line_filter(velocity.shape[3], M))
    components = [velocity[component] for component in range(3)]
    fields = jnp.stack(components + [components[a] * components[b] for a, b in factor_pairs])
    high = lax.Precision.HIGHEST
    third = jnp.einsum("fabk,mk->fabm", fields, matrix, precision=high)
    third = lax.all_to_all(third, "pz", split_axis=3, concat_axis=2, tiled=True)
    second = jnp.einsum("fabm,nb->fanm", third, matrix, precision=high)
    second = lax.all_to_all(second, "py", split_axis=2, concat_axis=1, tiled=True)
    coarse = jnp.einsum("fanm,pa->fnmp", second, matrix, precision=high)
    stress = jnp.stack(
        [coarse[3 + p] - coarse[a] * coarse[b] for p, (a, b) in enumerate(factor_pairs)]
    )
    return coarse[:3], stress


def shards(velocity):
    rows, columns = lax.axis_size("py"), lax.axis_size("pz")
    _, lines, depth, fine = velocity.shape
    whole_tiles = (
        M == LANES
        and lines % (2 * columns) == 0
        and depth % 16 == 0
        and (M // rows) % 8 == 0
        and (M // columns) % 8 == 0
        and rows * (lines // columns) <= LANES
    )
    return kernel_shards(velocity) if whole_tiles else plain_shards(velocity)


def solution(mesh):
    placed = P(None, "py", "pz", None)
    return jax.shard_map(
        shards, mesh=mesh, in_specs=(placed,), out_specs=(placed, placed), check_vma=False
    )
```

```python
import functools
import math

import jax
import jax.numpy as jnp
import ml_dtypes
import numpy as np
from jax import lax
from jax.experimental import pallas as pl
from jax.experimental.pallas import tpu as pltpu
from jax.sharding import PartitionSpec as P

M = 128

factor_pairs = ((0, 0), (0, 1), (0, 2), (1, 1), (1, 2), (2, 2))
fields_count = 9
LANES = 128


def line_filter(fine, coarse):
    half = coarse // 2
    modes = np.arange(1, half)
    width = 2.0 * math.pi / coarse
    gain = np.exp(-(modes.astype(np.float64) ** 2) * (width * width / 24.0))
    turns = np.arange(coarse)[:, None] * fine - np.arange(fine)[None, :] * coarse
    period = fine * coarse
    matrix = np.ones((coarse, fine))
    for mode, weight in zip(modes, gain):
        matrix += 2.0 * weight * np.cos(2.0 * math.pi * ((mode * turns) % period) / period)
    return (matrix / fine).astype(np.float32)


def halves(matrix):
    top = matrix.astype(ml_dtypes.bfloat16)
    return top, (matrix - top.astype(np.float32)).astype(ml_dtypes.bfloat16)


def split(value):
    top = value.astype(jnp.bfloat16)
    return top, (value - top.astype(jnp.float32)).astype(jnp.bfloat16)


def dot(left, right):
    return jnp.dot(left, right, preferred_element_type=jnp.float32)


def rows_times(value, table):
    width = table.shape[1] // 2
    top, rest = split(value)
    both = dot(top, table)
    return both[:, :width] + both[:, width:] + dot(rest, table[:, :width])


def kernel(
    rows, columns, velocity, third, second, first, filtered, stress,
    fine, lines, send_z, recv_z, send_y, recv_y, turned,
    load_sem, send_z_sem, recv_z_sem, send_y_sem, recv_y_sem,
):
    me_y = lax.axis_index("py")
    me_z = lax.axis_index("pz")
    steps = fine.shape[1]
    depth = fine.shape[3]
    block = LANES // columns
    band = filtered.shape[1]
    MESH = pl.DeviceIdType.MESH

    def load(c):
        return pltpu.make_async_copy(velocity.at[c], fine.at[c], load_sem.at[c])

    for c in range(3):
        load(c).start()

    barrier = pltpu.get_barrier_semaphore()
    for k in range(1, columns):
        pl.semaphore_signal(
            barrier, inc=1, device_id=(me_y, (me_z + k) % columns), device_id_type=MESH
        )
    for j in range(1, rows):
        pl.semaphore_signal(
            barrier, inc=1, device_id=((me_y + j) % rows, me_z), device_id_type=MESH
        )
    pl.semaphore_wait(barrier, columns + rows - 2)

    def copy_z(f, k, at=0, count=2):
        return pltpu.make_async_remote_copy(
            src_ref=send_z.at[f, k - 1, pl.ds(2 * at, count)],
            dst_ref=recv_z.at[f, k, pl.ds(2 * at, count)],
            send_sem=send_z_sem.at[f, k - 1],
            recv_sem=recv_z_sem.at[f, k - 1, at],
            device_id=(me_y, (me_z + k) % columns),
            device_id_type=MESH,
        )

    def copy_y(f, j, at=0, count=2):
        return pltpu.make_async_remote_copy(
            src_ref=send_y.at[f, j - 1, pl.ds(2 * at, count)],
            dst_ref=recv_y.at[f, pl.ds(j * steps + 2 * at, count)],
            send_sem=send_y_sem.at[f, j - 1],
            recv_sem=recv_y_sem.at[f, j - 1],
            device_id=((me_y + rows - j) % rows, me_z),
            device_id_type=MESH,
        )

    def pair_of(f):
        return f // 6 + f // 8, f - 3 - 2 * (f // 6) - f // 8

    half = steps // 2

    def contract_third(f, product):
        if product:
            left, right = pair_of(f)
        else:
            left = right = f

        def piece(t, carry):
            u, b = t // columns, t % columns
            where = pl.ds(2 * u, 2)
            value = fine[left, where, b]
            if product:
                value = value * fine[right, where, b]
            value = value.reshape(2 * depth, value.shape[-1])
            lines[b] = rows_times(value, third[b]).reshape(2, depth, LANES)
            return carry

        def regroup(u, i):
            group = lax.broadcasted_iota(jnp.int32, (depth, LANES), 1) // block
            parts = [lines[b, i] for b in range(columns)]
            for k in range(columns):
                out = parts[-1]
                for b in range(columns - 1):
                    out = jnp.where(group == (me_z + k + b) % columns, parts[b], out)
                if k == 0:
                    recv_z[f, 0, 2 * u + i] = out
                else:
                    send_z[f, k - 1, 2 * u + i] = out

        def unit(u, carry):
            lax.fori_loop(u * columns, (u + 1) * columns, piece, 0)
            for i in range(2):
                regroup(u, i)
            for k in range(1, columns):
                copy_z(f, k, u).start()
            return carry

        lax.fori_loop(0, half, unit, 0)

    def contract_second(f):
        def piece(h, carry):
            for k in range(1, columns):
                copy_z(f, k, h).wait_recv()
            value = jnp.concatenate(
                [recv_z[f, :, 2 * h + i].reshape(columns * depth, LANES) for i in range(2)], axis=1
            )
            top, rest = split(value)
            table = second[...]
            both = dot(table, top)
            out = both[:M] + both[M:] + dot(table[:M], rest)
            for i in range(2):
                for j in range(rows):
                    part = out[j * band : (j + 1) * band, i * LANES : (i + 1) * LANES]
                    if j == 0:
                        recv_y[f, 2 * h + i] = part
                    else:
                        send_y[f, j - 1, 2 * h + i] = part
            for j in range(1, rows):
                copy_y(f, j, h).start()
            return carry

        lax.fori_loop(0, half, piece, 0)

    def contract_first(f, product):
        for j in range(1, rows):
            copy_y(f, j, 0, steps).wait_recv()
        pad = jnp.zeros((LANES - rows * steps, LANES), jnp.float32)
        for m in range(band):
            plane = jnp.concatenate([recv_y[f, :, m, :], pad], axis=0).T
            for g in range(columns):
                turned[m * block : (m + 1) * block, g * LANES : (g + 1) * LANES] = plane[
                    g * block : (g + 1) * block
                ]
        out = rows_times(turned[...], first[...]).reshape(band, block, M)
        if product:
            left, right = pair_of(f)
            stress[f - 3] = out - filtered[left] * filtered[right]
        else:
            filtered[f] = out

    def loop(start, stop, *work):
        def body(f, carry):
            for one in work:
                one(f)
            return carry

        lax.fori_loop(start, stop, body, 0)

    loop(0, 3, lambda f: load(f).wait(), lambda f: contract_third(f, False))
    loop(3, fields_count, lambda f: contract_third(f, True))
    loop(0, 2, contract_second)
    loop(2, 5, contract_second, lambda f: contract_first(f - 2, False))
    loop(5, fields_count, contract_second, lambda f: contract_first(f - 2, True))
    loop(fields_count - 2, fields_count, lambda f: contract_first(f, True))

    def finish(f):
        for k in range(1, columns):
            copy_z(f, k, 0, steps).wait_send()
        for j in range(1, rows):
            copy_y(f, j, 0, steps).wait_send()

    loop(0, fields_count, finish)


def tables(fine, rows, columns):
    matrix = line_filter(fine, M)
    block, band, depth = M // columns, M // rows, fine // columns
    steps = fine // rows // columns
    top, rest = halves(matrix)
    third, second, first = [], [], []
    for b in range(columns):
        order = np.concatenate(
            [np.arange(block) + ((g - b) % columns) * block for g in range(columns)]
        )
        third.append(np.concatenate([top.T[:, order], rest.T[:, order]], axis=1))
    lines = np.concatenate([np.arange(band) + (-r % rows) * band for r in range(2 * rows)])
    for z in range(columns):
        order = np.concatenate(
            [np.arange(depth) + ((z - k) % columns) * depth for k in range(columns)]
        )
        second.append(np.stack([half[lines][:, order] for half in (top, rest)]))
        groups = []
        for g in range(columns):
            points = np.concatenate(
                [
                    (r % rows) * steps * columns + np.arange(steps) * columns + (g - z) % columns
                    for r in range(2 * rows)
                ]
            )
            groups.append(np.concatenate([top.T[points], rest.T[points]], axis=1))
        first.append(np.stack(groups))
    return np.stack(third), np.stack(second), np.stack(first)


def kernel_shards(velocity):
    rows, columns = lax.axis_size("py"), lax.axis_size("pz")
    me_y, me_z = lax.axis_index("py"), lax.axis_index("pz")
    _, lines, depth, fine = velocity.shape
    steps = lines // columns
    block, band = M // columns, M // rows
    third, second, first = tables(fine, rows, columns)
    second = lax.dynamic_slice(
        jnp.asarray(second), (me_z, 0, (rows - me_y) % rows * band, 0), (1, 2, M, fine)
    ).reshape(2 * M, fine)
    first = lax.dynamic_slice(
        jnp.asarray(first), (me_z, 0, me_y * steps, 0), (1, columns, rows * steps, 2 * M)
    )[0]
    first = jnp.pad(first, ((0, 0), (0, LANES - rows * steps), (0, 0)))
    first = first.reshape(columns * LANES, 2 * M)
    velocity = velocity.reshape(3, steps, columns, depth, fine)
    vmem = pl.BlockSpec(memory_space=pltpu.VMEM)
    dma = pltpu.SemaphoreType.DMA
    f32 = jnp.float32
    return pl.pallas_call(
        functools.partial(kernel, rows, columns),
        out_shape=(
            jax.ShapeDtypeStruct((3, band, block, M), f32),
            jax.ShapeDtypeStruct((6, band, block, M), f32),
        ),
        in_specs=[pl.BlockSpec(memory_space=pl.ANY), vmem, vmem, vmem],
        out_specs=(vmem, vmem),
        scratch_shapes=[
            pltpu.VMEM((3, steps, columns, depth, fine), f32),
            pltpu.VMEM((columns, 2, depth, LANES), f32),
            pltpu.VMEM((fields_count, columns - 1, steps, depth, LANES), f32),
            pltpu.VMEM((fields_count, columns, steps, depth, LANES), f32),
            pltpu.VMEM((fields_count, rows - 1, steps, band, LANES), f32),
            pltpu.VMEM((fields_count, rows * steps, band, LANES), f32),
            pltpu.VMEM((band * block, columns * LANES), f32),
            dma((3,)),
            dma((fields_count, columns - 1)),
            dma((fields_count, columns - 1, steps // 2)),
            dma((fields_count, rows - 1)),
            dma((fields_count, rows - 1)),
        ],
        compiler_params=pltpu.CompilerParams(
            collective_id=0, has_side_effects=True, vmem_limit_bytes=67_000_000
        ),
    )(velocity, jnp.asarray(third), second, first)


def plain_shards(velocity):
    matrix = jnp.asarray(line_filter(velocity.shape[3], M))
    components = [velocity[component] for component in range(3)]
    fields = jnp.stack(components + [components[a] * components[b] for a, b in factor_pairs])
    high = lax.Precision.HIGHEST
    third = jnp.einsum("fabk,mk->fabm", fields, matrix, precision=high)
    third = lax.all_to_all(third, "pz", split_axis=3, concat_axis=2, tiled=True)
    second = jnp.einsum("fabm,nb->fanm", third, matrix, precision=high)
    second = lax.all_to_all(second, "py", split_axis=2, concat_axis=1, tiled=True)
    coarse = jnp.einsum("fanm,pa->fnmp", second, matrix, precision=high)
    stress = jnp.stack(
        [coarse[3 + p] - coarse[a] * coarse[b] for p, (a, b) in enumerate(factor_pairs)]
    )
    return coarse[:3], stress


def shards(velocity):
    rows, columns = lax.axis_size("py"), lax.axis_size("pz")
    _, lines, depth, fine = velocity.shape
    whole_tiles = (
        M == LANES
        and lines % (2 * columns) == 0
        and depth % 16 == 0
        and (M // rows) % 8 == 0
        and (M // columns) % 8 == 0
        and rows * (lines // columns) <= LANES
    )
    return kernel_shards(velocity) if whole_tiles else plain_shards(velocity)


def solution(mesh):
    placed = P(None, "py", "pz", None)
    return jax.shard_map(
        shards, mesh=mesh, in_specs=(placed,), out_specs=(placed, placed), check_vma=False
    )
```

```python
import functools
import math

import jax
import jax.numpy as jnp
import ml_dtypes
import numpy as np
from jax import lax
from jax.experimental import pallas as pl
from jax.experimental.pallas import tpu as pltpu
from jax.sharding import PartitionSpec as P

M = 128

factor_pairs = ((0, 0), (0, 1), (0, 2), (1, 1), (1, 2), (2, 2))
fields_count = 9
LANES = 128


def line_filter(fine, coarse):
    half = coarse // 2
    modes = np.arange(1, half)
    width = 2.0 * math.pi / coarse
    gain = np.exp(-(modes.astype(np.float64) ** 2) * (width * width / 24.0))
    turns = np.arange(coarse)[:, None] * fine - np.arange(fine)[None, :] * coarse
    period = fine * coarse
    matrix = np.ones((coarse, fine))
    for mode, weight in zip(modes, gain):
        matrix += 2.0 * weight * np.cos(2.0 * math.pi * ((mode * turns) % period) / period)
    return (matrix / fine).astype(np.float32)


def halves(matrix):
    top = matrix.astype(ml_dtypes.bfloat16)
    return top, (matrix - top.astype(np.float32)).astype(ml_dtypes.bfloat16)


def split(value):
    top = value.astype(jnp.bfloat16)
    return top, (value - top.astype(jnp.float32)).astype(jnp.bfloat16)


def dot(left, right):
    return jnp.dot(left, right, preferred_element_type=jnp.float32)


def rows_times(value, table):
    width = table.shape[1] // 2
    top, rest = split(value)
    both = dot(top, table)
    return both[:, :width] + both[:, width:] + dot(rest, table[:, :width])


def kernel(
    rows, columns, velocity, third, second, first, filtered, stress,
    fine, lines, send_z, recv_z, send_y, recv_y, turned,
    load_sem, send_z_sem, recv_z_sem, send_y_sem, recv_y_sem,
):
    me_y = lax.axis_index("py")
    me_z = lax.axis_index("pz")
    steps = fine.shape[1]
    depth = fine.shape[3]
    block = LANES // columns
    band = filtered.shape[1]
    MESH = pl.DeviceIdType.MESH

    def load(c):
        return pltpu.make_async_copy(velocity.at[c], fine.at[c], load_sem.at[c])

    load(0).start()

    barrier = pltpu.get_barrier_semaphore()
    for k in range(1, columns):
        pl.semaphore_signal(
            barrier, inc=1, device_id=(me_y, (me_z + k) % columns), device_id_type=MESH
        )
    for j in range(1, rows):
        pl.semaphore_signal(
            barrier, inc=1, device_id=((me_y + j) % rows, me_z), device_id_type=MESH
        )
    pl.semaphore_wait(barrier, columns + rows - 2)

    def copy_z(f, k, at=0, count=2):
        return pltpu.make_async_remote_copy(
            src_ref=send_z.at[f, k - 1, pl.ds(2 * at, count)],
            dst_ref=recv_z.at[f, k, pl.ds(2 * at, count)],
            send_sem=send_z_sem.at[f, k - 1],
            recv_sem=recv_z_sem.at[f, k - 1, at],
            device_id=(me_y, (me_z + k) % columns),
            device_id_type=MESH,
        )

    def copy_y(f, j, at=0, count=2):
        return pltpu.make_async_remote_copy(
            src_ref=send_y.at[f, j - 1, pl.ds(2 * at, count)],
            dst_ref=recv_y.at[f, pl.ds(j * steps + 2 * at, count)],
            send_sem=send_y_sem.at[f, j - 1],
            recv_sem=recv_y_sem.at[f, j - 1],
            device_id=((me_y + rows - j) % rows, me_z),
            device_id_type=MESH,
        )

    def pair_of(f):
        return f // 6 + f // 8, f - 3 - 2 * (f // 6) - f // 8

    half = steps // 2

    def contract_third(f, product):
        if product:
            left, right = pair_of(f)
        else:
            left = right = f

        def piece(t, carry):
            u, b = t // columns, t % columns
            where = pl.ds(2 * u, 2)
            value = fine[left, where, b]
            if product:
                value = value * fine[right, where, b]
            value = value.reshape(2 * depth, value.shape[-1])
            lines[b] = rows_times(value, third[b]).reshape(2, depth, LANES)
            return carry

        def regroup(u, i):
            group = lax.broadcasted_iota(jnp.int32, (depth, LANES), 1) // block
            parts = [lines[b, i] for b in range(columns)]
            for k in range(columns):
                out = parts[-1]
                for b in range(columns - 1):
                    out = jnp.where(group == (me_z + k + b) % columns, parts[b], out)
                if k == 0:
                    recv_z[f, 0, 2 * u + i] = out
                else:
                    send_z[f, k - 1, 2 * u + i] = out

        def unit(u, carry):
            lax.fori_loop(u * columns, (u + 1) * columns, piece, 0)
            for i in range(2):
                regroup(u, i)
            for k in range(1, columns):
                copy_z(f, k, u).start()
            return carry

        lax.fori_loop(0, half, unit, 0)

    def contract_second(f):
        def piece(h, carry):
            for k in range(1, columns):
                copy_z(f, k, h).wait_recv()
            value = jnp.concatenate(
                [recv_z[f, :, 2 * h + i].reshape(columns * depth, LANES) for i in range(2)], axis=1
            )
            top, rest = split(value)
            table = second[...]
            both = dot(table, top)
            out = both[:M] + both[M:] + dot(table[:M], rest)
            for i in range(2):
                for j in range(rows):
                    part = out[j * band : (j + 1) * band, i * LANES : (i + 1) * LANES]
                    if j == 0:
                        recv_y[f, 2 * h + i] = part
                    else:
                        send_y[f, j - 1, 2 * h + i] = part
            for j in range(1, rows):
                copy_y(f, j, h).start()
            return carry

        lax.fori_loop(0, half, piece, 0)

    def contract_first(f, product):
        for j in range(1, rows):
            copy_y(f, j, 0, steps).wait_recv()
        pad = jnp.zeros((LANES - rows * steps, LANES), jnp.float32)
        for m in range(band):
            plane = jnp.concatenate([recv_y[f, :, m, :], pad], axis=0).T
            for g in range(columns):
                turned[m * block : (m + 1) * block, g * LANES : (g + 1) * LANES] = plane[
                    g * block : (g + 1) * block
                ]
        out = rows_times(turned[...], first[...]).reshape(band, block, M)
        if product:
            left, right = pair_of(f)
            stress[f - 3] = out - filtered[left] * filtered[right]
        else:
            filtered[f] = out

    def loop(start, stop, *work):
        def body(f, carry):
            for one in work:
                one(f)
            return carry

        lax.fori_loop(start, stop, body, 0)

    load(0).wait()
    for c in range(1, 3):
        load(c).start()
    contract_third(0, False)
    loop(1, 3, lambda f: load(f).wait(), lambda f: contract_third(f, False))
    loop(3, fields_count, lambda f: contract_third(f, True))
    loop(0, 2, contract_second)
    loop(2, 5, contract_second, lambda f: contract_first(f - 2, False))
    loop(5, fields_count, contract_second, lambda f: contract_first(f - 2, True))
    loop(fields_count - 2, fields_count, lambda f: contract_first(f, True))

    def finish(f):
        for k in range(1, columns):
            copy_z(f, k, 0, steps).wait_send()
        for j in range(1, rows):
            copy_y(f, j, 0, steps).wait_send()

    loop(0, fields_count, finish)


def tables(fine, rows, columns):
    matrix = line_filter(fine, M)
    block, band, depth = M // columns, M // rows, fine // columns
    steps = fine // rows // columns
    top, rest = halves(matrix)
    third, second, first = [], [], []
    for b in range(columns):
        order = np.concatenate(
            [np.arange(block) + ((g - b) % columns) * block for g in range(columns)]
        )
        third.append(np.concatenate([top.T[:, order], rest.T[:, order]], axis=1))
    lines = np.concatenate([np.arange(band) + (-r % rows) * band for r in range(2 * rows)])
    for z in range(columns):
        order = np.concatenate(
            [np.arange(depth) + ((z - k) % columns) * depth for k in range(columns)]
        )
        second.append(np.stack([half[lines][:, order] for half in (top, rest)]))
        groups = []
        for g in range(columns):
            points = np.concatenate(
                [
                    (r % rows) * steps * columns + np.arange(steps) * columns + (g - z) % columns
                    for r in range(2 * rows)
                ]
            )
            groups.append(np.concatenate([top.T[points], rest.T[points]], axis=1))
        first.append(np.stack(groups))
    return np.stack(third), np.stack(second), np.stack(first)


def kernel_shards(velocity):
    rows, columns = lax.axis_size("py"), lax.axis_size("pz")
    me_y, me_z = lax.axis_index("py"), lax.axis_index("pz")
    _, lines, depth, fine = velocity.shape
    steps = lines // columns
    block, band = M // columns, M // rows
    third, second, first = tables(fine, rows, columns)
    second = lax.dynamic_slice(
        jnp.asarray(second), (me_z, 0, (rows - me_y) % rows * band, 0), (1, 2, M, fine)
    ).reshape(2 * M, fine)
    first = lax.dynamic_slice(
        jnp.asarray(first), (me_z, 0, me_y * steps, 0), (1, columns, rows * steps, 2 * M)
    )[0]
    first = jnp.pad(first, ((0, 0), (0, LANES - rows * steps), (0, 0)))
    first = first.reshape(columns * LANES, 2 * M)
    velocity = velocity.reshape(3, steps, columns, depth, fine)
    vmem = pl.BlockSpec(memory_space=pltpu.VMEM)
    dma = pltpu.SemaphoreType.DMA
    f32 = jnp.float32
    return pl.pallas_call(
        functools.partial(kernel, rows, columns),
        out_shape=(
            jax.ShapeDtypeStruct((3, band, block, M), f32),
            jax.ShapeDtypeStruct((6, band, block, M), f32),
        ),
        in_specs=[pl.BlockSpec(memory_space=pl.ANY), vmem, vmem, vmem],
        out_specs=(vmem, vmem),
        scratch_shapes=[
            pltpu.VMEM((3, steps, columns, depth, fine), f32),
            pltpu.VMEM((columns, 2, depth, LANES), f32),
            pltpu.VMEM((fields_count, columns - 1, steps, depth, LANES), f32),
            pltpu.VMEM((fields_count, columns, steps, depth, LANES), f32),
            pltpu.VMEM((fields_count, rows - 1, steps, band, LANES), f32),
            pltpu.VMEM((fields_count, rows * steps, band, LANES), f32),
            pltpu.VMEM((band * block, columns * LANES), f32),
            dma((3,)),
            dma((fields_count, columns - 1)),
            dma((fields_count, columns - 1, steps // 2)),
            dma((fields_count, rows - 1)),
            dma((fields_count, rows - 1)),
        ],
        compiler_params=pltpu.CompilerParams(
            collective_id=0, has_side_effects=True, vmem_limit_bytes=67_000_000
        ),
    )(velocity, jnp.asarray(third), second, first)


def plain_shards(velocity):
    matrix = jnp.asarray(line_filter(velocity.shape[3], M))
    components = [velocity[component] for component in range(3)]
    fields = jnp.stack(components + [components[a] * components[b] for a, b in factor_pairs])
    high = lax.Precision.HIGHEST
    third = jnp.einsum("fabk,mk->fabm", fields, matrix, precision=high)
    third = lax.all_to_all(third, "pz", split_axis=3, concat_axis=2, tiled=True)
    second = jnp.einsum("fabm,nb->fanm", third, matrix, precision=high)
    second = lax.all_to_all(second, "py", split_axis=2, concat_axis=1, tiled=True)
    coarse = jnp.einsum("fanm,pa->fnmp", second, matrix, precision=high)
    stress = jnp.stack(
        [coarse[3 + p] - coarse[a] * coarse[b] for p, (a, b) in enumerate(factor_pairs)]
    )
    return coarse[:3], stress


def shards(velocity):
    rows, columns = lax.axis_size("py"), lax.axis_size("pz")
    _, lines, depth, fine = velocity.shape
    whole_tiles = (
        M == LANES
        and lines % (2 * columns) == 0
        and depth % 16 == 0
        and (M // rows) % 8 == 0
        and (M // columns) % 8 == 0
        and rows * (lines // columns) <= LANES
    )
    return kernel_shards(velocity) if whole_tiles else plain_shards(velocity)


def solution(mesh):
    placed = P(None, "py", "pz", None)
    return jax.shard_map(
        shards, mesh=mesh, in_specs=(placed,), out_specs=(placed, placed), check_vma=False
    )
```
